8 devices in a mesh: fsdp: 8 (over z, y, x, core).
Axes of the slice: x: 2, y: 2, z: 1, core: 2. Of those that a mesh axis runs over, the one named last changes fastest.
Arguments:
- hidden: bfloat16 [16384, 1280], P('fsdp')
- targets: int32 [16384], P('fsdp')
- resp_mask: int32 [16384], P('fsdp')
- resp_id: int32 [16384], P('fsdp')
- old_logp: float32 [16384], P('fsdp')
- ref_logp: float32 [16384], P('fsdp')
- rewards: float32 [128], P('fsdp')
- prompt_id: int32 [128], P('fsdp')
- norm_w: bfloat16 [1280], P('fsdp')
- embedding: bfloat16 [32000, 1280], P('fsdp')
Outputs:
- output 1: float32 [], replicated
- output 2: bfloat16 [16384, 1280], P('fsdp')
- output 3: float32 [32000, 1280], P('fsdp')
- output 4: float32 [1280], P('fsdp')
All inputs are finite; a program needn't handle non-finite values.
Results may differ from the reference program's by a relative error of at most 0.001.
Values are sent between devices in bfloat16 or wider.
A program may use at most 1 GiB of HBM per device.

```python
import jax
import jax.numpy as jnp
from jax import lax

NUM_SHARDS = 8
TOKENS_DEV = 2048
RESP_DEV = 16
GROUP_SIZE = 8
MODEL_DIM = 1280
VOCAB_SIZE = 32000

TOKENS_ALL = NUM_SHARDS * TOKENS_DEV
RESP_ALL = NUM_SHARDS * RESP_DEV
PROMPTS = RESP_ALL // GROUP_SIZE
TOK_BLOCK = min(TOKENS_DEV, 256)
CLIP_LOW = 0.8
CLIP_HIGH = 1.28
KL_COEF = 0.04
EPSILON = 1e-6


def norm_parts(hidden, norm_w):
    hid_f32 = hidden.astype(jnp.float32)
    inv_rms = lax.rsqrt(jnp.mean(hid_f32 * hid_f32, axis=-1, keepdims=True) + EPSILON)
    normed = hid_f32 * inv_rms
    x_rows = (normed * norm_w.astype(jnp.float32)).astype(jnp.bfloat16)
    return normed, inv_rms, x_rows


def token_logp(x_rows, targets, embedding):
    x_blocks = x_rows.reshape(-1, TOK_BLOCK, MODEL_DIM)
    tgt_blocks = targets.reshape(-1, TOK_BLOCK)

    def one_block(pair):
        x_block, tgt_block = pair
        logits = jnp.dot(x_block, embedding.T, preferred_element_type=jnp.float32)
        picked = jnp.take_along_axis(logits, tgt_block[:, None], axis=1)[:, 0]
        return picked - jax.nn.logsumexp(logits, axis=-1)

    return lax.map(one_block, (x_blocks, tgt_blocks)).reshape(-1)


def group_adv(rewards, prompt_id):
    rew_stats = jnp.stack([rewards, rewards * rewards, jnp.ones_like(rewards)], axis=1)
    totals = jax.ops.segment_sum(rew_stats, prompt_id, num_segments=PROMPTS)
    mean_r = totals[:, 0] / totals[:, 2]
    std_r = jnp.sqrt(jnp.maximum(totals[:, 1] / totals[:, 2] - mean_r * mean_r, 0.0))
    return (rewards - mean_r[prompt_id]) / (std_r[prompt_id] + EPSILON)


def token_terms(tok_logp, old_block, ref_block, adv_block):
    ratio = jnp.exp(tok_logp - old_block)
    surr_raw = ratio * adv_block
    surr_clip = jnp.clip(ratio, CLIP_LOW, CLIP_HIGH) * adv_block
    kl_gap = ref_block - tok_logp
    tok_loss = -jnp.minimum(surr_raw, surr_clip) + KL_COEF * (jnp.exp(kl_gap) - kl_gap - 1.0)
    keep = (surr_raw <= surr_clip) | ((ratio > CLIP_LOW) & (ratio < CLIP_HIGH))
    d_logp = -jnp.where(keep, surr_raw, 0.0) + KL_COEF * (1.0 - jnp.exp(kl_gap))
    return tok_loss, d_logp


def draw_layout(key):
    k_cut, k_cap, k_len = jax.random.split(key, 3)
    cuts = jnp.sort(jax.random.permutation(k_cut, TOKENS_DEV - 1)[:RESP_DEV - 1] + 1).astype(jnp.int32)
    tok_pos = jnp.arange(TOKENS_DEV, dtype=jnp.int32)
    resp_id = jnp.sum((tok_pos[:, None] >= cuts[None, :]).astype(jnp.int32), axis=1)
    starts = jnp.concatenate([jnp.zeros((1,), jnp.int32), cuts])
    len_cap = jax.random.randint(k_cap, (), 1, 2 * (TOKENS_DEV // RESP_DEV) + 1)
    prompt_len = jax.random.randint(k_len, (RESP_DEV,), 0, len_cap)
    in_resp = (tok_pos - starts[resp_id] >= prompt_len[resp_id]) | (tok_pos == TOKENS_DEV - 1)
    return resp_id, in_resp.astype(jnp.int32)


def draw_shift(key):
    k_kind, k_in, k_low, k_high = jax.random.split(key, 4)
    kind = jax.random.randint(k_kind, (TOKENS_ALL,), 0, 3)
    inside = jax.random.uniform(k_in, (TOKENS_ALL,), jnp.float32, -0.15, 0.15)
    below = jax.random.uniform(k_low, (TOKENS_ALL,), jnp.float32, -0.7, -0.3)
    above = jax.random.uniform(k_high, (TOKENS_ALL,), jnp.float32, 0.32, 0.7)
    return jnp.where(kind == 0, inside, jnp.where(kind == 1, below, above))


def setup_inputs(seed: int = 0) -> dict:
    key_list = jax.random.split(jax.random.key(seed), 9)
    resp_id, resp_mask = jax.vmap(draw_layout)(jax.random.split(key_list[0], NUM_SHARDS))
    prompt_id = (jax.random.permutation(key_list[1], RESP_ALL) // GROUP_SIZE).astype(jnp.int32)
    targets = jax.random.randint(key_list[2], (TOKENS_ALL,), 0, VOCAB_SIZE, dtype=jnp.int32)
    hidden = jax.random.normal(key_list[3], (TOKENS_ALL, MODEL_DIM), jnp.float32).astype(jnp.bfloat16)
    norm_w = (1.0 + 0.3 * jax.random.normal(key_list[4], (MODEL_DIM,), jnp.float32)).astype(jnp.bfloat16)
    embedding = (jax.random.normal(key_list[5], (VOCAB_SIZE, MODEL_DIM), jnp.float32) * MODEL_DIM ** -0.5).astype(jnp.bfloat16)
    rewards = jax.random.normal(key_list[6], (RESP_ALL,), jnp.float32)
    base_logp = token_logp(norm_parts(hidden, norm_w)[2], targets, embedding)
    old_logp = base_logp - draw_shift(key_list[7])
    ref_logp = base_logp + jax.random.uniform(key_list[8], (TOKENS_ALL,), jnp.float32, -2.5, 2.5)
    return {'hidden': hidden, 'targets': targets, 'resp_mask': resp_mask.reshape(-1), 'resp_id': resp_id.reshape(-1), 'old_logp': old_logp, 'ref_logp': ref_logp, 'rewards': rewards, 'prompt_id': prompt_id, 'norm_w': norm_w, 'embedding': embedding}


def reference(hidden, targets, resp_mask, resp_id, old_logp, ref_logp, rewards, prompt_id, norm_w, embedding):
    adv_resp = group_adv(rewards, prompt_id)
    owner = jnp.arange(TOKENS_ALL, dtype=jnp.int32) // TOKENS_DEV
    adv_tok = adv_resp[owner * RESP_DEV + resp_id]
    mask_f = resp_mask.astype(jnp.float32)
    count = jnp.sum(mask_f)
    normed, inv_rms, x_rows = norm_parts(hidden, norm_w)
    n_blocks = TOKENS_ALL // TOK_BLOCK
    vocab_ids = jnp.arange(VOCAB_SIZE, dtype=jnp.int32)

    def step(grad_emb, pack):
        x_block, tgt_block, mask_block, old_block, ref_block, adv_block = pack
        logits = jnp.dot(x_block, embedding.T, preferred_element_type=jnp.float32)
        log_norm = jax.nn.logsumexp(logits, axis=-1)
        tok_logp = jnp.take_along_axis(logits, tgt_block[:, None], axis=1)[:, 0] - log_norm
        tok_loss, d_logp = token_terms(tok_logp, old_block, ref_block, adv_block)
        tok_coef = mask_block * d_logp / count
        probs = jnp.exp(logits - log_norm[:, None])
        onehot = (vocab_ids[None, :] == tgt_block[:, None]).astype(jnp.float32)
        d_logits = (tok_coef[:, None] * (onehot - probs)).astype(jnp.bfloat16)
        dx_block = jnp.dot(d_logits, embedding, preferred_element_type=jnp.float32)
        grad_emb = grad_emb + jnp.dot(d_logits.T, x_block, preferred_element_type=jnp.float32)
        return grad_emb, (jnp.sum(mask_block * tok_loss), dx_block)

    pack = (x_rows.reshape(n_blocks, TOK_BLOCK, MODEL_DIM), targets.reshape(n_blocks, TOK_BLOCK), mask_f.reshape(n_blocks, TOK_BLOCK), old_logp.reshape(n_blocks, TOK_BLOCK), ref_logp.reshape(n_blocks, TOK_BLOCK), adv_tok.reshape(n_blocks, TOK_BLOCK))
    init_grad = jnp.zeros((VOCAB_SIZE, MODEL_DIM), jnp.float32)
    d_embedding, (loss_parts, dx_blocks) = lax.scan(step, init_grad, pack)
    d_x = dx_blocks.reshape(TOKENS_ALL, MODEL_DIM)
    d_norm_w = jnp.sum(d_x * normed, axis=0)
    d_normed = d_x * norm_w.astype(jnp.float32)
    d_hidden = (inv_rms * (d_normed - normed * jnp.mean(d_normed * normed, axis=-1, keepdims=True))).astype(jnp.bfloat16)
    mean_loss = jnp.sum(loss_parts) / count
    return mean_loss, d_hidden, d_embedding, d_norm_w
```

```python
import functools

import jax
import jax.numpy as jnp
from jax import lax
from jax.experimental import pallas as pl
from jax.experimental.pallas import tpu as pltpu
from jax.sharding import PartitionSpec as P

GROUP_SIZE = 8
CLIP_LOW = 0.8
CLIP_HIGH = 1.28
KL_COEF = 0.04
EPSILON = 1e-6

AXIS = 'fsdp'
N_DEV = 8
HALF = 256
BLK = 2 * HALF
N_J = 8
N_BLK = 4 * N_J
N_CHUNK = 5
SLAB = 16
N_SEND = 3
MESH = pl.DeviceIdType.MESH


def token_terms(tok_logp, old_block, ref_block, adv_block):
    ratio = jnp.exp(tok_logp - old_block)
    surr_raw = ratio * adv_block
    surr_clip = jnp.clip(ratio, CLIP_LOW, CLIP_HIGH) * adv_block
    kl_gap = ref_block - tok_logp
    tok_loss = -jnp.minimum(surr_raw, surr_clip) + KL_COEF * (jnp.exp(kl_gap) - kl_gap - 1.0)
    keep = (surr_raw <= surr_clip) | ((ratio > CLIP_LOW) & (ratio < CLIP_HIGH))
    d_logp = -jnp.where(keep, surr_raw, 0.0) + KL_COEF * (1.0 - jnp.exp(kl_gap))
    return tok_loss, d_logp


def bcast_kernel(x_ref, o_ref, send_sem, recv_sem):
    me = lax.axis_index(AXIS)
    barrier = pltpu.get_barrier_semaphore()
    for r in range(1, N_DEV):
        pl.semaphore_signal(barrier, inc=1, device_id=((me + r) % N_DEV,), device_id_type=MESH)
    pl.semaphore_wait(barrier, N_DEV - 1)
    copies = []
    for r in range(1, N_DEV):
        copies.append(pltpu.make_async_remote_copy(
            src_ref=x_ref, dst_ref=o_ref.at[me], send_sem=send_sem.at[r - 1], recv_sem=recv_sem.at[r - 1],
            device_id=((me + r) % N_DEV,), device_id_type=MESH))
    for c in copies:
        c.start()
    o_ref[me] = x_ref[...]
    for c in copies:
        c.wait()


def bcast_all(x, cid):
    return pl.pallas_call(
        bcast_kernel,
        out_shape=jax.ShapeDtypeStruct((N_DEV,) + x.shape, x.dtype),
        in_specs=[pl.BlockSpec(memory_space=pltpu.VMEM)],
        out_specs=pl.BlockSpec(memory_space=pltpu.VMEM),
        scratch_shapes=[pltpu.SemaphoreType.DMA((N_DEV - 1,)), pltpu.SemaphoreType.DMA((N_DEV - 1,))],
        compiler_params=pltpu.CompilerParams(collective_id=cid, has_side_effects=True),
        name=f'bcast{cid}',
    )(x)


def place(me):
    core = me % 2
    xpos = (me // 2) % 2
    ypos = me // 4
    par = (xpos + ypos) % 2
    pos = 2 * ypos + par
    partner = me + 1 - 2 * core
    xn = me + 2 - 4 * xpos
    yn = me + 4 - 8 * ypos
    nbr = ((1 - par) * xn + par * yn, par * xn + (1 - par) * yn)
    return core, me // 2, par, pos, partner, nbr


def logits_kernel(toki_ref, xown_hbm, e_hbm, xall_hbm, z_hbm, parts_ref,
                  e, z0, z1, xb0, xb1, acc, st,
                  e_sem, z_sem, xb_sem, oo_sem, ps, pr, ns, nr, fs, fr, qs, qr, ds, dr, ss, sr):
    vocab, dim = e_hbm.shape
    rows = vocab // N_CHUNK
    me = lax.axis_index(AXIS)
    core, chip, par_chip, pos, partner, nbr = place(me)
    diag_chip = 3 - chip
    diag = 2 * diag_chip + core
    zb = (z0, z1)
    xb = (xb0, xb1)

    barrier = pltpu.get_barrier_semaphore()
    for r in range(1, N_DEV):
        pl.semaphore_signal(barrier, inc=1, device_id=((me + r) % N_DEV,), device_id_type=MESH)
    pl.semaphore_wait(barrier, N_DEV - 1)

    def send(src, dst, ssem, rsem, dev):
        return pltpu.make_async_remote_copy(src_ref=src, dst_ref=dst, send_sem=ssem, recv_sem=rsem, device_id=(dev,), device_id_type=MESH)

    def to_partner(j):
        return send(xown_hbm.at[j], xall_hbm.at[me, j], ps.at[j], pr.at[j], partner)

    def to_nbr(side, j):
        return send(xown_hbm.at[j], xall_hbm.at[me, j], ns.at[side, j], nr.at[1 - side, j], nbr[side])

    def onward(side, j):
        ref = xall_hbm.at[nbr[1 - side], j]
        return send(ref, ref, fs.at[j], fr.at[j], nbr[side])

    def share_nbr(side, j):
        ref = xall_hbm.at[nbr[side], j]
        return send(ref, ref, qs.at[side, j], qr.at[side, j], partner)

    def share_diag(j):
        ref = xall_hbm.at[diag, j]
        return send(ref, ref, ds.at[j], dr.at[j], partner)

    def stats_group(g):
        return (chip, nbr[0] // 2, nbr[1] // 2, diag_chip)[g]

    def send_stats(r, g):
        rng = pl.ds(stats_group(g) * N_J, N_J)
        return send(st.at[rng], parts_ref.at[me, rng], ss.at[r - 1, g], sr.at[r - 1, g], (me + r) % N_DEV)

    e_copy = pltpu.make_async_copy(e_hbm, e, e_sem)
    e_copy.start()

    def load(par, half, src):
        return pltpu.make_async_copy(src, xb[par].at[half], xb_sem.at[par, half])

    def keep(par, j):
        return pltpu.make_async_copy(xb[par].at[core], xall_hbm.at[me, j], oo_sem.at[par])

    load(0, core, xown_hbm.at[0]).start()

    def first_sends(j, _):
        to_partner(j).start()
        to_nbr(0, j).start()
        to_nbr(1, j).start()
        return 0

    lax.fori_loop(0, N_J, first_sends, 0)
    to_partner(0).wait_recv()
    load(0, 1 - core, xall_hbm.at[partner, 0]).start()
    e_copy.wait()

    sub = lax.broadcasted_iota(jnp.int32, (SLAB, BLK), 0)

    def block_of(tt, par):
        a = tt // 4
        own = (3 - a) // 3
        far = a // 3
        near = 1 - own - far
        o = own * chip + near * (nbr[par] // 2) + far * diag_chip
        return o * N_J + own * (2 * tt + par) + near * (tt - 4) + far * (tt - 12 + 4 * par)

    def prefetch(tt, par):
        @pl.when(tt < 4)
        def _():
            j = 2 * tt + par
            load(par, core, xown_hbm.at[j]).start()
            to_partner(j).wait_recv()
            load(par, 1 - core, xall_hbm.at[partner, j]).start()

        @pl.when((tt >= 4) & (tt < 12))
        def _():
            j = tt - 4
            load(par, core, xall_hbm.at[nbr[par], j]).start()
            share_nbr(par, j).wait_recv()
            load(par, 1 - core, xall_hbm.at[nbr[par] + 1 - 2 * core, j]).start()

        @pl.when(tt >= 12)
        def _():
            j = tt - 12 + 4 * par
            load(par, core, xall_hbm.at[diag, j]).start()
            share_diag(j).wait_recv()
            load(par, 1 - core, xall_hbm.at[diag + 1 - 2 * core, j]).start()

    def z_out(blk, par):
        return pltpu.make_async_copy(zb[par], z_hbm.at[blk], z_sem.at[par])

    def dot(par, v, x):
        zb[par][v * rows:(v + 1) * rows, :] = lax.dot_general(
            e[v * rows:(v + 1) * rows, :], x, (((1,), (1,)), ((), ())), preferred_element_type=jnp.float32)

    def stats(par, v, rel, m, s, zt):
        cm = m
        for a in range(rows // SLAB):
            r0 = v * rows + a * SLAB
            cm = jnp.maximum(cm, zb[par][r0:r0 + SLAB, :])
        s = s * jnp.exp(m - cm)
        for a in range(rows // SLAB):
            r0 = v * rows + a * SLAB
            z = zb[par][r0:r0 + SLAB, :]
            s = s + jnp.exp(z - cm)
            zt = zt + jnp.where(rel == r0, z, 0.0)
        return cm, s, zt

    def close(par, blk):
        rel = jnp.broadcast_to(toki_ref[blk, 0:1, :], (SLAB, BLK)) - sub
        m, s, zt = stats(par, N_CHUNK - 1, rel, acc[0], acc[1], acc[2])
        top = jnp.max(m, axis=0, keepdims=True)
        st[blk, 0:1, :] = top + jnp.log(jnp.sum(s * jnp.exp(m - top), axis=0, keepdims=True))
        st[blk, 1:2, :] = jnp.sum(zt, axis=0, keepdims=True)

    def pair(tt, _):
        for par in (0, 1):
            other = 1 - par
            blk = block_of(tt, par)
            if par == 1:
                @pl.when((tt >= 1) & (tt < 9))
                def _():
                    j = tt - 1
                    for side in (0, 1):
                        to_nbr(1 - side, j).wait_recv()
                    for side in (0, 1):
                        share_nbr(side, j).start()

                    @pl.when(j < 4)
                    def _():
                        onward(0, j).start()

                    @pl.when(j >= 4)
                    def _():
                        onward(1, j).start()

                @pl.when((tt >= 10) & (tt < 14))
                def _():
                    for half in (0, 4):
                        onward(0, tt - 10 + half).wait_recv()
                        share_diag(tt - 10 + half).start()

                @pl.when(tt == 4)
                def _():
                    for r in range(1, N_DEV):
                        send_stats(r, 0).start()

                @pl.when(tt == 12)
                def _():
                    for r in range(1, N_DEV):
                        send_stats(r, 1).start()
                        send_stats(r, 2).start()

            for half in (0, 1):
                load(par, half, xown_hbm.at[0]).wait()

            @pl.when(tt < 4)
            def _():
                keep(par, 2 * tt + par).start()

            if par == 0:
                @pl.when((tt >= 1) & (tt < 5))
                def _():
                    keep(1, 0).wait()

                prefetch(tt, 1)
            else:
                @pl.when(tt < 4)
                def _():
                    keep(0, 0).wait()

                @pl.when(tt < 15)
                def _():
                    prefetch(tt + 1, 0)

            @pl.when(tt >= 1)
            def _():
                z_out(blk, par).wait()

            x = xb[par][...].reshape(BLK, dim)
            dot(par, 0, x)
            close(other, block_of(tt, 0) if par == 1 else block_of((tt + 15) % 16, 1))
            rel = jnp.broadcast_to(toki_ref[blk, 0:1, :], (SLAB, BLK)) - sub
            m = jnp.full((SLAB, BLK), -jnp.inf, jnp.float32)
            s = jnp.zeros((SLAB, BLK), jnp.float32)
            zt = s
            for v in range(1, N_CHUNK):
                dot(par, v, x)
                m, s, zt = stats(par, v - 1, rel, m, s, zt)
            acc[0] = m
            acc[1] = s
            acc[2] = zt
            z_out(blk, par).start()
        return 0

    lax.fori_loop(0, N_BLK // 2, pair, 0)
    close(1, block_of(15, 1))
    for r in range(1, N_DEV):
        send_stats(r, 3).start()
    parts_ref[me] = st[...]

    def drain(j, _):
        to_partner(j).wait_send()
        for side in (0, 1):
            to_nbr(side, j).wait_send()
            share_nbr(side, j).wait_send()
        onward(0, j).wait_send()
        share_diag(j).wait_send()
        return 0

    lax.fori_loop(0, N_J, drain, 0)
    for par in (0, 1):
        z_out(0, par).wait()
    for r in range(1, N_DEV):
        for g in range(4):
            send_stats(r, g).wait()


def logits_pass(toki, x_own, emb):
    vocab, dim = emb.shape
    vm = pltpu.VMEM
    dma = pltpu.SemaphoreType.DMA
    any_spec = pl.BlockSpec(memory_space=pl.ANY)
    vmem_spec = pl.BlockSpec(memory_space=pltpu.VMEM)
    return pl.pallas_call(
        logits_kernel,
        in_specs=[vmem_spec, any_spec, any_spec],
        out_specs=[any_spec, any_spec, vmem_spec],
        out_shape=[
            jax.ShapeDtypeStruct((N_DEV, N_J, HALF, dim), jnp.bfloat16),
            jax.ShapeDtypeStruct((N_BLK, vocab, BLK), jnp.float32),
            jax.ShapeDtypeStruct((N_DEV, N_BLK, 2, BLK), jnp.float32),
        ],
        scratch_shapes=[
            vm((vocab, dim), jnp.bfloat16), vm((vocab, BLK), jnp.float32), vm((vocab, BLK), jnp.float32),
            vm((2, HALF, dim), jnp.bfloat16), vm((2, HALF, dim), jnp.bfloat16),
            vm((3, SLAB, BLK), jnp.float32), vm((N_BLK, 2, BLK), jnp.float32),
            dma, dma((2,)), dma((2, 2)), dma((2,)),
            dma((N_J,)), dma((N_J,)), dma((2, N_J)), dma((2, N_J)), dma((N_J,)), dma((N_J,)),
            dma((2, N_J)), dma((2, N_J)), dma((N_J,)), dma((N_J,)), dma((N_DEV - 1, 4)), dma((N_DEV - 1, 4)),
        ],
        compiler_params=pltpu.CompilerParams(collective_id=1, has_side_effects=True, vmem_limit_bytes=60_000_000),
        cost_estimate=pl.CostEstimate(flops=2 * N_BLK * BLK * vocab * dim, bytes_accessed=4 * N_BLK * BLK * vocab, transcendentals=0),
        name='logits_pass',
    )(toki, x_own, emb)


def grad_kernel(tokf_ref, toki_ref, x_hbm, z_hbm, et_hbm, de_hbm, dx_hbm, ring_hbm,
                et, de, dz0, dz1, zb, xb0, xb1, dx0, dx1, d2d0, d2d1, rb0, rb1, sb,
                et_sem, x_sem, z_sem, d2d_ssem, d2d_rsem, ring_ssem, ring_rsem, rb_sem, out_sem, de_sem):
    dim, vocab = et_hbm.shape
    rows = vocab // N_CHUNK
    mrow = dim // N_CHUNK
    me = lax.axis_index(AXIS)
    core, chip, par, pos, partner, nbr = place(me)
    dz = (dz0, dz1)
    xb = (xb0, xb1)
    dx = (dx0, dx1)
    d2d = (d2d0, d2d1)
    rb = (rb0, rb1)

    barrier = pltpu.get_barrier_semaphore()
    for peer in (partner, nbr[0], nbr[1]):
        pl.semaphore_signal(barrier, inc=1, device_id=(peer,), device_id_type=MESH)
    pl.semaphore_wait(barrier, 3)

    def owner_of(stream, slot):
        p = (pos + 3 - slot) % 4 if stream == 0 else (pos + 1 + slot) % 4
        yy = p // 2
        return 2 * yy + (p % 2 + yy) % 2

    def block_of(stream, cnt):
        return owner_of(stream, cnt // 4) * N_J + 4 * stream + cnt % 4

    def x_copy(stream, cnt):
        o = owner_of(stream, cnt // 4)
        return pltpu.make_async_copy(x_hbm.at[pl.ds(2 * o, 2), 4 * stream + cnt % 4], xb[stream], x_sem.at[stream])

    def z_copy(g, slot):
        t = (g // N_CHUNK) % N_BLK
        cnt = t // 2
        odd = t % 2
        blk = (1 - odd) * block_of(0, cnt) + odd * block_of(1, cnt)
        part = g % N_CHUNK
        return pltpu.make_async_copy(z_hbm.at[blk, pl.ds(pl.multiple_of(part * rows, 8), rows)], zb.at[slot], z_sem.at[slot])

    et_copy = pltpu.make_async_copy(et_hbm, et, et_sem)
    z_copy(0, 0).start()
    z_copy(1, 1).start()
    et_copy.start()
    x_copy(0, 0).start()

    sub = lax.broadcasted_iota(jnp.int32, (SLAB, BLK), 0)

    def make_dz(dst, blk, v, slot):
        lse = jnp.broadcast_to(tokf_ref[blk, 0:1, :], (SLAB, BLK))
        coef = jnp.broadcast_to(tokf_ref[blk, 1:2, :], (SLAB, BLK))
        rel = jnp.broadcast_to(toki_ref[blk, 0:1, :], (SLAB, BLK)) - sub - v * rows
        for a in range(rows // SLAB):
            p = jnp.exp(zb[slot, a * SLAB:(a + 1) * SLAB, :] - lse)
            hot = jnp.where(rel == a * SLAB, 1.0, 0.0)
            dst[pl.ds(pl.multiple_of(v * rows + a * SLAB, SLAB), SLAB), :] = (coef * (hot - p)).astype(jnp.bfloat16)

    def first(v, _):
        slot = v % 2
        z_copy(v, slot).wait()
        make_dz(dz0, block_of(0, 0), v, slot)
        z_copy(v + 2, slot).start()
        return 0

    lax.fori_loop(0, N_CHUNK, first, 0)

    def clear(r, _):
        de[pl.ds(pl.multiple_of(r * 80, 8), 80), :] = jnp.zeros((80, dim), jnp.float32)
        return 0

    lax.fori_loop(0, vocab // 80, clear, 0)
    et_copy.wait()

    def d2d_copy(stream):
        return pltpu.make_async_remote_copy(
            src_ref=dx[stream].at[1 - core], dst_ref=d2d[stream], send_sem=d2d_ssem.at[stream], recv_sem=d2d_rsem.at[stream],
            device_id=(partner,), device_id_type=MESH)

    def ring_copy(stream, cnt, buf):
        return pltpu.make_async_remote_copy(
            src_ref=sb.at[stream, buf], dst_ref=ring_hbm.at[stream, cnt], send_sem=ring_ssem.at[stream, buf], recv_sem=ring_rsem.at[stream, cnt],
            device_id=(nbr[stream],), device_id_type=MESH)

    def fetch_copy(stream, cnt):
        return pltpu.make_async_copy(ring_hbm.at[stream, cnt], rb[stream], rb_sem.at[stream])

    def out_copy(stream, i, buf):
        return pltpu.make_async_copy(sb.at[stream, buf], dx_hbm.at[4 * stream + i], out_sem.at[stream, buf])

    def finish(stream, cnt):
        buf = cnt % N_SEND
        d2d_copy(stream).wait()

        @pl.when((cnt >= N_SEND) & (cnt < 12 + N_SEND))
        def _():
            ring_copy(stream, 0, buf).wait_send()

        @pl.when(cnt >= 12 + N_SEND)
        def _():
            out_copy(stream, 0, buf).wait()

        def add(r, with_ring):
            sl = pl.ds(pl.multiple_of(r * 64, 8), 64)
            val = dx[stream][core, sl, :] + d2d[stream][sl, :]
            if with_ring:
                val = val + rb[stream][sl, :]
            sb[stream, buf, sl, :] = val
            return 0

        @pl.when(cnt < 4)
        def _():
            lax.fori_loop(0, dim // 64, lambda r, c: add(r, False), 0)

        @pl.when(cnt >= 4)
        def _():
            fetch_copy(stream, cnt - 4).wait()
            lax.fori_loop(0, dim // 64, lambda r, c: add(r, True), 0)

        @pl.when(cnt < 12)
        def _():
            ring_copy(stream, cnt, buf).start()

        @pl.when(cnt >= 12)
        def _():
            out_copy(stream, cnt - 12, buf).start()

    def pair(cnt, _):
        for stream in (0, 1):
            t = 2 * cnt + stream
            other = 1 - stream
            x_copy(stream, cnt).wait()
            if stream == 0:
                x_copy(1, cnt).start()
                nblk = block_of(1, cnt)
            else:
                @pl.when(cnt < 15)
                def _():
                    x_copy(0, cnt + 1).start()
                nblk = block_of(0, (cnt + 1) % 16)

            def chunk(v, _):
                g = (t + 1) * N_CHUNK + v
                slot = g % 2
                z_copy(g, slot).wait()
                xv = xb[stream][...].reshape(BLK, dim)
                sl = pl.ds(pl.multiple_of(v * rows, SLAB), rows)
                de[sl, :] += jnp.dot(dz[stream][sl, :], xv, preferred_element_type=jnp.float32)
                ml = pl.ds(pl.multiple_of(v * mrow, 16), mrow)
                part = jnp.dot(et[ml, :], dz[stream][...], preferred_element_type=jnp.float32)
                dx[stream][0, ml, :] = part[:, :HALF]
                dx[stream][1, ml, :] = part[:, HALF:]
                make_dz(dz[other], nblk, v, slot)
                z_copy(g + 2, slot).start()
                return 0

            lax.fori_loop(0, N_CHUNK, chunk, 0)

            if stream == 1:
                finish(0, cnt)
            else:
                @pl.when(cnt > 0)
                def _():
                    finish(1, cnt - 1)
            d2d_copy(stream).start()

            @pl.when(cnt >= 4)
            def _():
                ring_copy(stream, cnt - 4, 0).wait_recv()
                fetch_copy(stream, cnt - 4).start()
        return 0

    lax.fori_loop(0, 16, pair, 0)
    de_copy = pltpu.make_async_copy(de, de_hbm, de_sem)
    de_copy.start()
    finish(1, 15)
    for stream in (0, 1):
        for cnt in range(16 - N_SEND, 16):
            out_copy(stream, 0, cnt % N_SEND).wait()
    last = (N_BLK + 1) * N_CHUNK
    for g in (last, last + 1):
        z_copy(g, g % 2).wait()
    de_copy.wait()


def grad_pass(tokf, toki, x_all, z_all, emb_t):
    dim, vocab = emb_t.shape
    rows = vocab // N_CHUNK
    f32 = jnp.float32
    vm = pltpu.VMEM
    dma = pltpu.SemaphoreType.DMA
    piece = (dim, HALF)
    return pl.pallas_call(
        grad_kernel,
        in_specs=[pl.BlockSpec(memory_space=pltpu.VMEM)] * 2 + [pl.BlockSpec(memory_space=pl.ANY)] * 3,
        out_specs=[pl.BlockSpec(memory_space=pl.ANY)] * 3,
        out_shape=[
            jax.ShapeDtypeStruct((vocab, dim), f32),
            jax.ShapeDtypeStruct((N_J,) + piece, f32),
            jax.ShapeDtypeStruct((2, 12) + piece, f32),
        ],
        scratch_shapes=[
            vm((dim, vocab), jnp.bfloat16), vm((vocab, dim), f32),
            vm((vocab, BLK), jnp.bfloat16), vm((vocab, BLK), jnp.bfloat16),
            vm((2, rows, BLK), f32),
            vm((2, HALF, dim), jnp.bfloat16), vm((2, HALF, dim), jnp.bfloat16),
            vm((2,) + piece, f32), vm((2,) + piece, f32),
            vm(piece, f32), vm(piece, f32), vm(piece, f32), vm(piece, f32),
            vm((2, N_SEND) + piece, f32),
            dma, dma((2,)), dma((2,)), dma((2,)), dma((2,)), dma((2, N_SEND)), dma((2, 12)), dma((2,)), dma((2, N_SEND)), dma,
        ],
        compiler_params=pltpu.CompilerParams(collective_id=2, has_side_effects=True, vmem_limit_bytes=67_000_000),
        cost_estimate=pl.CostEstimate(flops=4 * N_BLK * BLK * vocab * dim, bytes_accessed=4 * N_BLK * BLK * vocab, transcendentals=0),
        name='grad_pass',
    )(tokf, toki, x_all, z_all, emb_t)


def solution(mesh):
    shards = mesh.shape[AXIS]

    def local(hidden, targets, resp_mask, resp_id, old_logp, ref_logp, rewards, prompt_id, norm_w, embedding):
        tok_dev, dim = hidden.shape
        vocab = embedding.shape[0]
        n_resp = rewards.shape[0]
        prompts = n_resp * shards // GROUP_SIZE
        me = lax.axis_index(AXIS)
        f32 = jnp.float32

        pieces = [targets.astype(f32), resp_mask.astype(f32), resp_id.astype(f32), old_logp, ref_logp]
        tail = jnp.concatenate([rewards, prompt_id.astype(f32), norm_w.astype(f32)])
        tail = jnp.pad(tail, (0, 1024 - tail.shape[0]))
        small = jnp.concatenate(pieces + [tail]).reshape(-1, 128)
        every = bcast_all(small, 0).reshape(shards, -1)
        tgt, mask_f, rid, old, ref = [every[:, i * tok_dev:(i + 1) * tok_dev] for i in range(5)]
        tail = every[:, 5 * tok_dev:]
        rew = tail[:, :n_resp]
        pid = tail[:, n_resp:2 * n_resp].astype(jnp.int32)
        gain = tail[:, 2 * n_resp:2 * n_resp + norm_w.shape[0]].reshape(dim)

        hid_f32 = hidden.astype(f32)
        inv_rms = lax.rsqrt(jnp.mean(hid_f32 * hid_f32, axis=-1, keepdims=True) + EPSILON)
        normed = hid_f32 * inv_rms
        x_rows = (normed * gain).astype(jnp.bfloat16)

        same = (pid.reshape(-1)[:, None] == jnp.arange(prompts, dtype=jnp.int32)[None, :])
        flat = rew.reshape(-1)[:, None]
        tot1 = jnp.sum(jnp.where(same, flat, 0.0), axis=0)
        tot2 = jnp.sum(jnp.where(same, flat * flat, 0.0), axis=0)
        cnt = jnp.sum(jnp.where(same, 1.0, 0.0), axis=0)
        mean_r = tot1 / cnt
        std_r = jnp.sqrt(jnp.maximum(tot2 / cnt - mean_r * mean_r, 0.0))
        mean_t = jnp.sum(jnp.where(same, mean_r[None, :], 0.0), axis=1)
        std_t = jnp.sum(jnp.where(same, std_r[None, :], 0.0), axis=1)
        adv = ((rew.reshape(-1) - mean_t) / (std_t + EPSILON)).reshape(shards, n_resp)
        hit = rid[:, None, :] == jnp.arange(n_resp, dtype=f32)[None, :, None]
        adv_tok = jnp.sum(jnp.where(hit, adv[:, :, None], 0.0), axis=1)
        count = jnp.sum(mask_f)

        def order(a):
            return a.reshape(shards // 2, 2, N_J, HALF).transpose(0, 2, 1, 3).reshape(N_BLK, BLK)

        tgt_loc = order(tgt).astype(jnp.int32) - me * vocab
        toki = jnp.broadcast_to(tgt_loc[:, None, :], (N_BLK, 8, BLK))

        x_all, z_all, parts = logits_pass(toki, x_rows.reshape(N_J, HALF, dim), embedding)
        lses = parts[:, :, 0]
        top = jnp.max(lses, axis=0)
        lse = top + jnp.log(jnp.sum(jnp.exp(lses - top), axis=0))
        tok_logp = jnp.sum(parts[:, :, 1], axis=0) - lse
        mask_b = order(mask_f)
        tok_loss, d_logp = token_terms(tok_logp, order(old), order(ref), order(adv_tok))
        coef = mask_b * d_logp / count
        mean_loss = jnp.sum(mask_b * tok_loss) / count
        tokf = jnp.concatenate([lse[:, None], coef[:, None], jnp.zeros((N_BLK, 6, BLK), f32)], axis=1)

        d_embedding, dx_t, _ = grad_pass(tokf, toki, x_all, z_all, embedding.T)
        d_x = dx_t.transpose(0, 2, 1).reshape(tok_dev, dim)
        dg_part = jnp.pad(jnp.sum(d_x * normed, axis=0), (0, 2048 - dim)).reshape(16, 128)
        dg_all = jnp.sum(bcast_all(dg_part, 3), axis=0).reshape(-1)[:dim].reshape(shards, dim // shards)
        d_norm_w = lax.dynamic_index_in_dim(dg_all, me, 0, keepdims=False)
        d_normed = d_x * gain
        d_hidden = (inv_rms * (d_normed - normed * jnp.mean(d_normed * normed, axis=-1, keepdims=True))).astype(jnp.bfloat16)
        return mean_loss, d_hidden, d_embedding, d_norm_w

    tok_spec = P(AXIS)
    row_spec = P(AXIS, None)
    return jax.shard_map(local, mesh=mesh, in_specs=(row_spec, tok_spec, tok_spec, tok_spec, tok_spec, tok_spec, tok_spec, tok_spec, tok_spec, row_spec), out_specs=(P(), row_spec, row_spec, tok_spec), check_vma=False)
```

```python
import functools

import jax
import jax.numpy as jnp
from jax import lax
from jax.experimental import pallas as pl
from jax.experimental.pallas import tpu as pltpu
from jax.sharding import PartitionSpec as P

GROUP_SIZE = 8
CLIP_LOW = 0.8
CLIP_HIGH = 1.28
KL_COEF = 0.04
EPSILON = 1e-6

AXIS = 'fsdp'
N_DEV = 8
PEERS = range(1, N_DEV)
N_PEER = len(PEERS)
PAIR = (0, 1)
ORIGIN = (0, 0, 0)
NONE = 0
SIDE_VMEM = 48_000_000
HALF = 256
BLK = 2 * HALF
LANES = 128
N_J = 8
N_BLK = 4 * N_J
N_CHUNK = 5
SLAB = 16
N_SEND = 3
N_PIECE = 2
SLABS_E = (12, 12)
SLABS_X = (6, 6, 6, 8)
N_LOGIT = 10
K_PART = 1024
MESH = pl.DeviceIdType.MESH
NT_DIMS = (((1,), (1,)), ((), ()))
PARAMS = functools.partial(pltpu.CompilerParams, has_side_effects=True)


row_mean = functools.partial(jnp.mean, axis=-1, keepdims=True)
col_sum = functools.partial(jnp.sum, axis=0, keepdims=True)


def token_terms(tok_logp, old_block, ref_block, adv_block):
    ratio = jnp.exp(tok_logp - old_block)
    surr_raw = ratio * adv_block
    surr_clip = jnp.clip(ratio, CLIP_LOW, CLIP_HIGH) * adv_block
    kl_gap = ref_block - tok_logp
    tok_loss = -jnp.minimum(surr_raw, surr_clip) + KL_COEF * (jnp.exp(kl_gap) - kl_gap - 1.0)
    keep = (surr_raw <= surr_clip) | ((ratio > CLIP_LOW) & (ratio < CLIP_HIGH))
    d_logp = -jnp.where(keep, surr_raw, 0.0) + KL_COEF * (1.0 - jnp.exp(kl_gap))
    return tok_loss, d_logp


def bcast_kernel(x_ref, o_ref, send_sem, recv_sem):
    me = lax.axis_index(AXIS)
    barrier = pltpu.get_barrier_semaphore()
    for r in PEERS:
        pl.semaphore_signal(barrier, device_id=((me + r) % N_DEV,), device_id_type=MESH)
    pl.semaphore_wait(barrier, N_PEER)
    copies = []
    for r in PEERS:
        copies.append(pltpu.make_async_remote_copy(
            src_ref=x_ref, dst_ref=o_ref.at[me], send_sem=send_sem.at[r - 1], recv_sem=recv_sem.at[r - 1],
            device_id=((me + r) % N_DEV,), device_id_type=MESH))
    for c in copies:
        c.start()
    o_ref[me] = x_ref[...]
    for c in copies:
        c.wait()


def bcast_all(x, cid):
    return pl.pallas_call(
        bcast_kernel,
        out_shape=jax.ShapeDtypeStruct((N_DEV,) + x.shape, x.dtype),
        in_specs=[pl.BlockSpec(memory_space=pltpu.VMEM)],
        out_specs=pl.BlockSpec(memory_space=pltpu.VMEM),
        scratch_shapes=[pltpu.SemaphoreType.DMA((N_PEER,)), pltpu.SemaphoreType.DMA((N_PEER,))],
        compiler_params=PARAMS(collective_id=cid),
        name=f'bcast{cid}',
    )(x)


def place(me):
    core = me % 2
    xpos = (me // 2) % 2
    ypos = me // 4
    par = (xpos + ypos) % 2
    pos = 2 * ypos + par
    partner = me + 1 - 2 * core
    xn = me + 2 - 4 * xpos
    yn = me + 4 - 8 * ypos
    nbr = ((1 - par) * xn + par * yn, par * xn + (1 - par) * yn)
    return core, me // 2, par, pos, partner, nbr


def logits_kernel(toki_ref, xown_hbm, e_hbm, xall_hbm, z_hbm, parts_ref, et_hbm,
                  e, zb, xb0, xb1, acc, st, eb,
                  eb_sem, e_sem, z_sem, xb_sem, oo_sem, ps, pr, ns, nr, fs, fr, qs, qr, ds, dr, ss, sr):
    vocab, dim = e_hbm.shape
    rows = vocab // N_LOGIT
    me = lax.axis_index(AXIS)
    core, chip, par_chip, pos, partner, nbr = place(me)
    diag_chip = 3 - chip
    diag = 2 * diag_chip + core
    xb = (xb0, xb1)

    barrier = pltpu.get_barrier_semaphore()
    for r in PEERS:
        pl.semaphore_signal(barrier, device_id=((me + r) % N_DEV,), device_id_type=MESH)
    pl.semaphore_wait(barrier, N_PEER)

    def send(src, dst, ssem, rsem, dev):
        return pltpu.make_async_remote_copy(src_ref=src, dst_ref=dst, send_sem=ssem, recv_sem=rsem, device_id=(dev,), device_id_type=MESH)

    def to_partner(j):
        return send(xown_hbm.at[j], xall_hbm.at[me, j], ps.at[j], pr.at[j], partner)

    def to_nbr(side, j):
        return send(xown_hbm.at[j], xall_hbm.at[me, j], ns.at[side, j], nr.at[1 - side, j], nbr[side])

    def onward(side, j):
        ref = xall_hbm.at[nbr[1 - side], j]
        return send(ref, ref, fs.at[j], fr.at[j], nbr[side])

    def share_nbr(side, j):
        ref = xall_hbm.at[nbr[side], j]
        return send(ref, ref, qs.at[side, j], qr.at[side, j], partner)

    def share_diag(j):
        ref = xall_hbm.at[diag, j]
        return send(ref, ref, ds.at[j], dr.at[j], partner)

    def stats_group(g):
        return (chip, nbr[0] // 2, nbr[1] // 2, diag_chip)[g]

    def send_stats(r, g):
        rng = pl.ds(stats_group(g) * N_J, N_J)
        return send(st.at[rng], parts_ref.at[me, rng], ss.at[r - 1, g], sr.at[r - 1, g], (me + r) % N_DEV)

    e_copy = pltpu.make_async_copy(e_hbm, e.at[pl.ds(0, vocab)], e_sem)
    e[vocab:, :] = jnp.zeros((e.shape[0] - vocab, dim), jnp.bfloat16)
    e_copy.start()

    def load(par, half, src):
        return pltpu.make_async_copy(src, xb[par].at[half], xb_sem.at[par, half])

    def keep(par, j):
        return pltpu.make_async_copy(xb[par].at[core], xall_hbm.at[me, j], oo_sem.at[par])

    load(0, core, xown_hbm.at[0]).start()

    def first_sends(j, _):
        to_partner(j).start()
        to_nbr(0, j).start()
        to_nbr(1, j).start()
        return 0

    lax.fori_loop(0, N_J, first_sends, 0)
    to_partner(0).wait_recv()
    load(0, 1 - core, xall_hbm.at[partner, 0]).start()
    e_copy.wait()

    sub = lax.broadcasted_iota(jnp.int32, (SLAB, BLK), 0)

    def block_of(tt, par):
        a = tt // 4
        own = (3 - a) // 3
        far = a // 3
        near = 1 - own - far
        o = own * chip + near * (nbr[par] // 2) + far * diag_chip
        return o * N_J + own * (2 * tt + par) + near * (tt - 4) + far * (tt - 12 + 4 * par)

    def prefetch(tt, par):
        @pl.when(tt < 4)
        def _():
            j = 2 * tt + par
            load(par, core, xown_hbm.at[j]).start()
            to_partner(j).wait_recv()
            load(par, 1 - core, xall_hbm.at[partner, j]).start()

        @pl.when((tt >= 4) & (tt < 12))
        def _():
            j = tt - 4
            load(par, core, xall_hbm.at[nbr[par], j]).start()
            share_nbr(par, j).wait_recv()
            load(par, 1 - core, xall_hbm.at[nbr[par] + 1 - 2 * core, j]).start()

        @pl.when(tt >= 12)
        def _():
            j = tt - 12 + 4 * par
            load(par, core, xall_hbm.at[diag, j]).start()
            share_diag(j).wait_recv()
            load(par, 1 - core, xall_hbm.at[diag + 1 - 2 * core, j]).start()

    def z_out(blk, par):
        return pltpu.make_async_copy(zb.at[pl.ds(par * vocab, vocab)], z_hbm.at[blk], z_sem.at[par])

    def part_of(base, q, a):
        return pl.ds(pl.multiple_of(base + q * rows + a * SLAB, SLAB), SLAB)

    def et_out(t, par):
        return pltpu.make_async_copy(eb.at[par], et_hbm.at[:, pl.ds(pl.multiple_of(t * LANES, LANES), LANES)], eb_sem.at[par])

    def dot(base, q, x):
        zb[pl.ds(pl.multiple_of(base + q * rows, SLAB), rows), :] = lax.dot_general(
            e[q * rows:(q + 1) * rows, :], x, NT_DIMS, preferred_element_type=jnp.float32)

    def stats(base, q, rel, m, s, zt):
        cm = m
        for a in range(rows // SLAB):
            cm = jnp.maximum(cm, zb[part_of(base, q, a), :])
        s = s * jnp.exp(m - cm)
        for a in range(rows // SLAB):
            z = zb[part_of(base, q, a), :]
            s = s + jnp.exp(z - cm)
            zt = zt + jnp.where(rel == q * rows + a * SLAB, z, 0.0)
        return cm, s, zt

    def close(base, blk):
        rel = jnp.broadcast_to(toki_ref[blk, 0:1, :], (SLAB, BLK)) - sub
        m, s, zt = stats(base, N_LOGIT - 1, rel, acc[0], acc[1], acc[2])
        top = jnp.max(m, axis=0, keepdims=True)
        st[blk, 0:1, :] = top + jnp.log(col_sum(s * jnp.exp(m - top)))
        st[blk, 1:2, :] = col_sum(zt)

    def pair(tt, _):
        for par in PAIR:
            blk = block_of(tt, par)
            if par == 1:
                @pl.when((tt >= 2) & (tt < 10))
                def _():
                    j = tt - 2
                    for side in PAIR:
                        to_nbr(1 - side, j).wait_recv()
                    for side in PAIR:
                        share_nbr(side, j).start()

                    @pl.when(j < 4)
                    def _():
                        onward(0, j).start()

                    @pl.when(j >= 4)
                    def _():
                        onward(1, j).start()

                @pl.when((tt >= 10) & (tt < 14))
                def _():
                    for half in (0, 4):
                        onward(0, tt - 10 + half).wait_recv()
                        share_diag(tt - 10 + half).start()

                @pl.when(tt == 4)
                def _():
                    for r in PEERS:
                        send_stats(r, 0).start()

                @pl.when(tt == 12)
                def _():
                    for r in PEERS:
                        send_stats(r, 1).start()
                        send_stats(r, 2).start()

            for half in PAIR:
                load(par, half, xown_hbm.at[0]).wait()

            @pl.when(tt < 4)
            def _():
                keep(par, 2 * tt + par).start()

            if par == 0:
                @pl.when((tt >= 1) & (tt < 5))
                def _():
                    keep(1, 0).wait()

                prefetch(tt, 1)
            else:
                @pl.when(tt < 4)
                def _():
                    keep(0, 0).wait()

                @pl.when(tt < 15)
                def _():
                    prefetch(tt + 1, 0)

            @pl.when(tt >= 1)
            def _():
                z_out(blk, par).wait()
                et_out(0, par).wait()

            x = xb[par][...].reshape(BLK, dim)
            t = 2 * tt + par
            cur = (5 * t) % 2 * vocab
            same = cur + me // N_DEV * SLAB
            dot(cur, 0, x)
            eb[par] = e[pl.ds(pl.multiple_of(t * LANES, LANES), LANES), :].T
            close((5 * t + 5) % 2 * vocab + me // N_DEV * SLAB, block_of(tt, 0) if par == 1 else block_of((tt + 15) % 16, 1))
            rel = jnp.broadcast_to(toki_ref[blk, 0:1, :], (SLAB, BLK)) - sub
            m = jnp.full((SLAB, BLK), -jnp.inf, jnp.float32)
            s = jnp.zeros((SLAB, BLK), jnp.float32)
            zt = s
            for q in range(1, N_LOGIT):
                dot(cur, q, x)
                m, s, zt = stats(same, q - 1, rel, m, s, zt)
            acc[0] = m
            acc[1] = s
            acc[2] = zt
            z_out(blk, par).start()
            et_out(t, par).start()
        return 0

    lax.fori_loop(0, N_BLK // 2, pair, 0)
    close(vocab, block_of(15, 1))
    for r in PEERS:
        send_stats(r, 3).start()
    parts_ref[me] = st[...]

    def drain(j, _):
        to_partner(j).wait_send()
        for side in PAIR:
            to_nbr(side, j).wait_send()
            share_nbr(side, j).wait_send()
        onward(0, j).wait_send()
        share_diag(j).wait_send()
        return 0

    lax.fori_loop(0, N_J, drain, 0)
    for par in PAIR:
        z_out(0, par).wait()
        et_out(0, par).wait()
    for r in PEERS:
        for g in range(4):
            send_stats(r, g).wait()


def logits_pass(toki, x_own, emb):
    vocab, dim = emb.shape
    vm = pltpu.VMEM
    dma = pltpu.SemaphoreType.DMA
    two = dma((2,))
    any_spec = pl.BlockSpec(memory_space=pl.ANY)
    vmem_spec = pl.BlockSpec(memory_space=pltpu.VMEM)
    return pl.pallas_call(
        logits_kernel,
        in_specs=[vmem_spec, any_spec, any_spec],
        out_specs=[any_spec, any_spec, vmem_spec, any_spec],
        out_shape=[
            jax.ShapeDtypeStruct((N_DEV, N_J, HALF, dim), jnp.bfloat16),
            jax.ShapeDtypeStruct((N_BLK, vocab, BLK), jnp.float32),
            jax.ShapeDtypeStruct((N_DEV, N_BLK, 2, BLK), jnp.float32),
            jax.ShapeDtypeStruct((dim, N_BLK * LANES), jnp.bfloat16),
        ],
        scratch_shapes=[
            vm((N_BLK * LANES, dim), jnp.bfloat16), vm((2 * vocab, BLK), jnp.float32),
            *[vm((2, HALF, dim), jnp.bfloat16)] * 2,
            vm((3, SLAB, BLK), jnp.float32), vm((N_BLK, 2, BLK), jnp.float32), vm((2, dim, LANES), jnp.bfloat16),
            two, dma, two, dma((2, 2)), two,
            dma((N_J,)), dma((N_J,)), *[dma((2, N_J))] * 2, dma((N_J,)), dma((N_J,)),
            *[dma((2, N_J))] * 2, dma((N_J,)), dma((N_J,)), dma((N_PEER, 4)), dma((N_PEER, 4)),
        ],
        compiler_params=PARAMS(collective_id=1, vmem_limit_bytes=60_000_000),
        cost_estimate=pl.CostEstimate(flops=2 * N_BLK * BLK * vocab * dim, bytes_accessed=4 * N_BLK * BLK * vocab, transcendentals=NONE),
        name='logits_pass',
    )(toki, x_own, emb)


def grad_kernel(tokf_ref, toki_ref, x_hbm, z_hbm, et_hbm, de_hbm, dx_hbm, ring_hbm, dz_hbm, xl_hbm,
                et, de, dz, zb, xb0, xb1, dx0, dx1, d2d0, d2d1, rb0, rb1, sb,
                et_sem, x_sem, z_sem, d2d_ssem, d2d_rsem, ring_ssem, ring_rsem, rb_sem, out_sem, de_sem, held_sem):
    dim, vocab = et_hbm.shape[0], z_hbm.shape[1]
    rows = vocab // N_CHUNK
    mrow = dim // N_CHUNK
    piece = rows // N_PIECE
    n_slab = rows // SLAB
    me = lax.axis_index(AXIS)
    core, chip, par, pos, partner, nbr = place(me)
    xb = (xb0, xb1)
    dx = (dx0, dx1)
    d2d = (d2d0, d2d1)
    rb = (rb0, rb1)

    barrier = pltpu.get_barrier_semaphore()
    for peer in (partner, nbr[0], nbr[1]):
        pl.semaphore_signal(barrier, device_id=(peer,), device_id_type=MESH)
    pl.semaphore_wait(barrier, 3)

    def owner_of(stream, slot):
        p = (pos + 3 - slot) % 4 if stream == 0 else (pos + 1 + slot) % 4
        yy = p // 2
        return 2 * yy + (p % 2 + yy) % 2

    def block_of(stream, cnt):
        return owner_of(stream, cnt // 4) * N_J + 4 * stream + cnt % 4

    def x_copy(stream, cnt):
        o = owner_of(stream, cnt // 4)
        return pltpu.make_async_copy(x_hbm.at[pl.ds(2 * o, 2), 4 * stream + cnt % 4], xb[stream], x_sem.at[stream])

    def z_copy(g, slot):
        t = (g // N_CHUNK) % N_BLK
        cnt = t // 2
        odd = t % 2
        blk = (1 - odd) * block_of(0, cnt) + odd * block_of(1, cnt)
        part = g % N_CHUNK
        return pltpu.make_async_copy(z_hbm.at[blk, pl.ds(pl.multiple_of(part * rows, 8), rows)], zb.at[slot], z_sem.at[slot])

    et_copy = pltpu.make_async_copy(et_hbm, et, et_sem)
    z_copy(0, 0).start()
    z_copy(1, 1).start()
    et_copy.start()
    x_copy(0, 0).start()

    sub = lax.broadcasted_iota(jnp.int32, (SLAB, BLK), 0)

    def make_dz(base, blk, v, slot, slabs):
        lse = jnp.broadcast_to(tokf_ref[blk, 0:1, :], (SLAB, BLK))
        coef = jnp.broadcast_to(tokf_ref[blk, 1:2, :], (SLAB, BLK))
        rel = jnp.broadcast_to(toki_ref[blk, 0:1, :], (SLAB, BLK)) - sub - v * rows
        for a in slabs:
            p = jnp.exp(zb[slot, a * SLAB:(a + 1) * SLAB, :] - lse)
            hot = jnp.where(rel == a * SLAB, 1.0, 0.0)
            dz[pl.ds(pl.multiple_of(base + v * rows + a * SLAB, SLAB), SLAB), :] = (coef * (hot - p)).astype(jnp.bfloat16)

    def first(v, _):
        slot = v % 2
        z_copy(v, slot).wait()
        make_dz(0, block_of(0, 0), v, slot, range(n_slab))
        z_copy(v + 2, slot).start()
        return 0

    lax.fori_loop(0, N_CHUNK, first, 0)

    def clear(r, _):
        de[pl.ds(pl.multiple_of(r * 80, 8), 80), :] = jnp.zeros((80, dim), jnp.float32)
        return 0

    lax.fori_loop(0, vocab // 80, clear, 0)
    et_copy.wait()

    def d2d_copy(stream):
        return pltpu.make_async_remote_copy(
            src_ref=dx[stream].at[1 - core], dst_ref=d2d[stream], send_sem=d2d_ssem.at[stream], recv_sem=d2d_rsem.at[stream],
            device_id=(partner,), device_id_type=MESH)

    def ring_copy(stream, cnt, buf):
        return pltpu.make_async_remote_copy(
            src_ref=sb.at[stream, buf], dst_ref=ring_hbm.at[stream, cnt], send_sem=ring_ssem.at[stream, buf], recv_sem=ring_rsem.at[stream, cnt],
            device_id=(nbr[stream],), device_id_type=MESH)

    def fetch_copy(stream, cnt):
        return pltpu.make_async_copy(ring_hbm.at[stream, cnt], rb[stream], rb_sem.at[stream])

    def out_copy(stream, i, buf):
        return pltpu.make_async_copy(sb.at[stream, buf], dx_hbm.at[4 * stream + i], out_sem.at[stream, buf])

    def finish(stream, cnt):
        buf = cnt % N_SEND
        d2d_copy(stream).wait()

        @pl.when((cnt >= N_SEND) & (cnt < 12 + N_SEND))
        def _():
            ring_copy(stream, 0, buf).wait_send()

        @pl.when(cnt >= 12 + N_SEND)
        def _():
            out_copy(stream, 0, buf).wait()

        def add(r, with_ring):
            sl = pl.ds(pl.multiple_of(r * 64, 8), 64)
            val = dx[stream][core, sl, :] + d2d[stream][sl, :]
            if with_ring:
                val = val + rb[stream][sl, :]
            sb[stream, buf, sl, :] = val
            return 0

        @pl.when(cnt < 4)
        def _():
            lax.fori_loop(0, dim // 64, lambda r, c: add(r, False), 0)

        @pl.when(cnt >= 4)
        def _():
            fetch_copy(stream, cnt - 4).wait()
            lax.fori_loop(0, dim // 64, lambda r, c: add(r, True), 0)

        @pl.when(cnt < 12)
        def _():
            ring_copy(stream, cnt, buf).start()

        @pl.when(cnt >= 12)
        def _():
            out_copy(stream, cnt - 12, buf).start()

    def pair(cnt, _):
        for stream in PAIR:
            t = 2 * cnt + stream
            cur = (5 * t) % 2 * vocab
            nxt = (5 * t + 5) % 2 * vocab
            x_copy(stream, cnt).wait()
            if stream == 0:
                x_copy(1, cnt).start()
                nblk = block_of(1, cnt)
            else:
                x_copy(0, cnt + 1).start()
                nblk = block_of(0, cnt + 1)

            def chunk(v, _):
                g = (t + 1) * N_CHUNK + v
                slot = g % 2
                z_copy(g, slot).wait()
                xv = xb[stream][...].reshape(BLK, dim)
                ml = pl.ds(pl.multiple_of(v * mrow, 16), mrow)
                cut = 0
                for q in range(N_PIECE):
                    sl = pl.ds(pl.multiple_of(v * rows + q * piece, SLAB), piece)
                    lhs = dz[pl.ds(pl.multiple_of(cur + v * rows + q * piece, SLAB), piece), :]
                    de[sl, :] += jnp.dot(lhs, xv, preferred_element_type=jnp.float32)
                    make_dz(nxt, nblk, v, slot, range(cut, cut + SLABS_E[q]))
                    cut += SLABS_E[q]
                part = jnp.zeros((mrow, BLK), jnp.float32)
                for q in range(len(SLABS_X)):
                    lo = q * K_PART
                    hi = min(lo + K_PART, vocab)
                    rhs = dz[pl.ds(pl.multiple_of(cur + lo, SLAB), hi - lo), :]
                    part = part + jnp.dot(et[ml, lo:hi], rhs, preferred_element_type=jnp.float32)
                    make_dz(nxt, nblk, v, slot, range(cut, cut + SLABS_X[q]))
                    cut += SLABS_X[q]
                assert cut == n_slab
                dx[stream][0, ml, :] = part[:, :HALF]
                dx[stream][1, ml, :] = part[:, HALF:]
                z_copy(g + 2, slot).start()
                return 0

            lax.fori_loop(0, N_CHUNK, chunk, 0)

            if stream == 1:
                finish(0, cnt)
            else:
                @pl.when(cnt > 0)
                def _():
                    finish(1, cnt - 1)
            d2d_copy(stream).start()

            @pl.when(cnt >= 4)
            def _():
                ring_copy(stream, cnt - 4, 0).wait_recv()
                fetch_copy(stream, cnt - 4).start()
        return 0

    lax.fori_loop(0, 15, pair, 0)
    de_copy = pltpu.make_async_copy(de, de_hbm, de_sem)
    de_copy.start()
    held = []
    for stream in PAIR:
        x_copy(stream, 15).wait()
        if stream == 0:
            x_copy(1, 15).start()
        cur = stream * vocab
        held.append(pltpu.make_async_copy(dz.at[pl.ds(cur, vocab)], dz_hbm.at[stream], held_sem.at[0, stream]))
        held.append(pltpu.make_async_copy(xb[stream], xl_hbm.at[stream], held_sem.at[1, stream]))
        for c in held[-2:]:
            c.start()

        def last_chunk(v, _):
            ml = pl.ds(pl.multiple_of(v * mrow, 16), mrow)
            part = jnp.dot(et[ml, :vocab], dz[cur:cur + vocab, :], preferred_element_type=jnp.float32)
            dx[stream][0, ml, :] = part[:, :HALF]
            dx[stream][1, ml, :] = part[:, HALF:]
            if stream == 0:
                g = 31 * N_CHUNK + v
                slot = g % 2
                z_copy(g, slot).wait()
                make_dz(vocab, block_of(1, 15), v, slot, range(n_slab))

                @pl.when(v < N_CHUNK - 2)
                def _():
                    z_copy(g + 2, slot).start()
            return 0

        lax.fori_loop(0, N_CHUNK, last_chunk, 0)
        finish(1 - stream, 14 + stream)
        d2d_copy(stream).start()
        ring_copy(stream, 11, 0).wait_recv()
        fetch_copy(stream, 11).start()
    finish(1, 15)
    for c in held:
        c.wait()
    for stream in PAIR:
        for cnt in range(16 - N_SEND, 16):
            out_copy(stream, 0, cnt % N_SEND).wait()
    de_copy.wait()


def grad_pass(tokf, toki, x_all, z_all, emb_t):
    dim, vocab = emb_t.shape[0], z_all.shape[1]
    rows = vocab // N_CHUNK
    f32 = jnp.float32
    vm = pltpu.VMEM
    dma = pltpu.SemaphoreType.DMA
    two = dma((2,))
    piece = (dim, HALF)
    by_buf = dma((2, N_SEND))
    return pl.pallas_call(
        grad_kernel,
        in_specs=[pl.BlockSpec(memory_space=pltpu.VMEM)] * 2 + [pl.BlockSpec(memory_space=pl.ANY)] * 3,
        out_specs=[pl.BlockSpec(memory_space=pl.ANY)] * 5,
        out_shape=[
            jax.ShapeDtypeStruct((vocab, dim), f32),
            jax.ShapeDtypeStruct((N_J,) + piece, f32),
            jax.ShapeDtypeStruct((2, 12) + piece, f32),
            jax.ShapeDtypeStruct((2, vocab, BLK), jnp.bfloat16),
            jax.ShapeDtypeStruct((2, 2, HALF, dim), jnp.bfloat16),
        ],
        scratch_shapes=[
            vm(emb_t.shape, jnp.bfloat16), vm((vocab, dim), f32),
            vm((2 * vocab, BLK), jnp.bfloat16),
            vm((2, rows, BLK), f32),
            *[vm((2, HALF, dim), jnp.bfloat16)] * 2,
            *[vm((2,) + piece, f32)] * 2,
            *[vm(piece, f32)] * 4,
            vm((2, N_SEND) + piece, f32),
            dma, two, two, two, two, by_buf, dma((2, 12)), two, by_buf, dma, dma((2, 2)),
        ],
        compiler_params=PARAMS(collective_id=2, vmem_limit_bytes=67_000_000),
        cost_estimate=pl.CostEstimate(flops=4 * N_BLK * BLK * vocab * dim, bytes_accessed=4 * N_BLK * BLK * vocab, transcendentals=NONE),
        name='grad_pass',
    )(tokf, toki, x_all, z_all, emb_t)


def emb_kernel(part_ref, dz_ref, x_ref, o_ref):
    acc = part_ref[...]
    for b in PAIR:
        acc = acc + jnp.dot(dz_ref[b], x_ref[b], preferred_element_type=jnp.float32)
    o_ref[...] = acc


def emb_pass(de_part, dz_last, x_last):
    vocab, dim = de_part.shape
    rows = vocab // 10
    return pl.pallas_call(
        emb_kernel,
        grid=(10,),
        in_specs=[
            pl.BlockSpec((rows, dim), lambda i: (i, 0)),
            pl.BlockSpec((2, rows, BLK), lambda i: (0, i, 0)),
            pl.BlockSpec((2, BLK, dim), lambda i: ORIGIN),
        ],
        out_specs=pl.BlockSpec((rows, dim), lambda i: (i, 0)),
        out_shape=jax.ShapeDtypeStruct((vocab, dim), jnp.float32),
        compiler_params=pltpu.CompilerParams(vmem_limit_bytes=SIDE_VMEM),
        cost_estimate=pl.CostEstimate(flops=4 * BLK * vocab * dim, bytes_accessed=8 * vocab * dim, transcendentals=NONE),
        name='emb_pass',
    )(de_part, dz_last, x_last)


def norm_kernel(dx_ref, h_ref, g_ref, dh_ref, dg_ref):
    dim = h_ref.shape[-1]
    dx = dx_ref[0].T
    hid = h_ref[0].astype(jnp.float32)
    inv = lax.rsqrt(row_mean(hid * hid) + EPSILON)
    n = hid * inv
    part = jnp.sum((dx * n).reshape(HALF // 8, 8, dim), axis=0)

    @pl.when(pl.program_id(0) == 0)
    def _():
        dg_ref[...] = part

    @pl.when(pl.program_id(0) > 0)
    def _():
        dg_ref[...] += part

    u = dx * g_ref[...]
    dh_ref[0] = (inv * (u - n * row_mean(u * n))).astype(jnp.bfloat16)


def norm_pass(dx_t, hid, gain):
    n_j, dim, half = dx_t.shape
    return pl.pallas_call(
        norm_kernel,
        grid=(n_j,),
        in_specs=[
            pl.BlockSpec((1, dim, half), lambda j: (j, 0, 0)),
            pl.BlockSpec((1, half, dim), lambda j: (j, 0, 0)),
            pl.BlockSpec((1, dim), lambda j: ORIGIN[1:]),
        ],
        out_specs=[
            pl.BlockSpec((1, half, dim), lambda j: (j, 0, 0)),
            pl.BlockSpec((8, dim), lambda j: ORIGIN[1:]),
        ],
        out_shape=[
            jax.ShapeDtypeStruct((n_j, half, dim), jnp.bfloat16),
            jax.ShapeDtypeStruct((8, dim), jnp.float32),
        ],
        compiler_params=pltpu.CompilerParams(vmem_limit_bytes=SIDE_VMEM),
        name='norm_pass',
    )(dx_t, hid, gain)


def solution(mesh):
    shards = mesh.shape[AXIS]

    def local(hidden, targets, resp_mask, resp_id, old_logp, ref_logp, rewards, prompt_id, norm_w, embedding):
        tok_dev, dim = hidden.shape
        vocab = embedding.shape[0]
        n_resp = rewards.shape[0]
        prompts = n_resp * shards // GROUP_SIZE
        me = lax.axis_index(AXIS)
        f32 = jnp.float32

        pieces = [targets.astype(f32), resp_mask.astype(f32), resp_id.astype(f32), old_logp, ref_logp]
        tail = jnp.concatenate([rewards, prompt_id.astype(f32), norm_w.astype(f32)])
        tail = jnp.pad(tail, (0, 1024 - tail.size))
        small = jnp.concatenate(pieces + [tail]).reshape(-1, 128)
        every = bcast_all(small, 0).reshape(shards, -1)
        tgt, mask_f, rid, old, ref = [every[:, i * tok_dev:(i + 1) * tok_dev] for i in range(5)]
        tail = every[:, 5 * tok_dev:]
        rew = tail[:, :n_resp]
        pid = tail[:, n_resp:2 * n_resp].astype(jnp.int32)
        gain = tail[:, 2 * n_resp:2 * n_resp + norm_w.shape[0]].reshape(dim)

        hid_f32 = hidden.astype(f32)
        inv_rms = lax.rsqrt(row_mean(hid_f32 * hid_f32) + EPSILON)
        normed = hid_f32 * inv_rms
        x_rows = (normed * gain).astype(jnp.bfloat16)

        same = (pid.reshape(-1)[:, None] == jnp.arange(prompts, dtype=jnp.int32)[None, :])
        flat = rew.reshape(-1)[:, None]
        tot1 = jnp.sum(jnp.where(same, flat, 0.0), axis=0)
        tot2 = jnp.sum(jnp.where(same, flat * flat, 0.0), axis=0)
        cnt = jnp.sum(jnp.where(same, 1.0, 0.0), axis=0)
        mean_r = tot1 / cnt
        std_r = jnp.sqrt(jnp.maximum(tot2 / cnt - mean_r * mean_r, 0.0))
        mean_t = jnp.sum(jnp.where(same, mean_r[None, :], 0.0), axis=1)
        std_t = jnp.sum(jnp.where(same, std_r[None, :], 0.0), axis=1)
        adv = ((rew.reshape(-1) - mean_t) / (std_t + EPSILON)).reshape(shards, n_resp)
        hit = rid[:, None, :] == jnp.arange(n_resp, dtype=f32)[None, :, None]
        adv_tok = jnp.sum(jnp.where(hit, adv[:, :, None], 0.0), axis=1)
        count = jnp.sum(mask_f)

        def order(a):
            return a.reshape(shards // 2, 2, N_J, HALF).transpose(0, 2, 1, 3).reshape(N_BLK, BLK)

        tgt_loc = order(tgt).astype(jnp.int32) - me * vocab
        toki = jnp.broadcast_to(tgt_loc[:, None, :], (N_BLK, 8, BLK))

        x_all, z_all, parts, emb_t = logits_pass(toki, x_rows.reshape(N_J, HALF, dim), embedding)
        lses = parts[:, :, 0]
        top = jnp.max(lses, axis=0)
        lse = top + jnp.log(jnp.sum(jnp.exp(lses - top), axis=0))
        tok_logp = jnp.sum(parts[:, :, 1], axis=0) - lse
        mask_b = order(mask_f)
        tok_loss, d_logp = token_terms(tok_logp, order(old), order(ref), order(adv_tok))
        coef = mask_b * d_logp / count
        mean_loss = jnp.sum(mask_b * tok_loss) / count
        tokf = jnp.concatenate([lse[:, None], coef[:, None], jnp.zeros((N_BLK, 6, BLK), f32)], axis=1)

        de_part, dx_t, _, dz_last, x_last = grad_pass(tokf, toki, x_all, z_all, emb_t)
        d_hidden, dg_rows = norm_pass(dx_t, hidden.reshape(N_J, HALF, dim), gain.reshape(1, dim))
        d_hidden = d_hidden.reshape(tok_dev, dim)
        dg_part = jnp.pad(jnp.sum(dg_rows, axis=0), (0, 2048 - dim)).reshape(16, 128)
        d_embedding = emb_pass(de_part, dz_last, x_last.reshape(2, BLK, dim))
        dg_all = jnp.sum(bcast_all(dg_part, 3), axis=0).reshape(-1)[:dim].reshape(shards, dim // shards)
        d_norm_w = lax.dynamic_index_in_dim(dg_all, me, 0, keepdims=False)
        return mean_loss, d_hidden, d_embedding, d_norm_w

    tok_spec = P(AXIS)
    row_spec = P(AXIS, None)
    return jax.shard_map(local, mesh=mesh, in_specs=(row_spec, tok_spec, tok_spec, tok_spec, tok_spec, tok_spec, tok_spec, tok_spec, tok_spec, row_spec), out_specs=(P(), row_spec, row_spec, tok_spec), check_vma=False)
```
